32 devices in a mesh: tm: 8 (over z, y), col: 4 (over x, core).
Axes of the slice: x: 2, y: 2, z: 4, core: 2. Of those that a mesh axis runs over, the one named last changes fastest.
Arguments:
- block_values: bfloat16 [4, 16384, 128], P('col', 'tm'), may hold values from -6 to 6
- block_shifts: bfloat16 [4, 16384, 128], P('col', 'tm'), may hold values from -1 to 1
- block_sensor: int32 [4, 16384], P('col', 'tm'), may hold values from 0 to 4095
- block_window: int32 [4, 16384], P('col', 'tm'), may hold values from 0 to 3
- block_owner: int32 [4, 16384, 1], P('col', 'tm'), may hold values from 0 to 7; in each aligned block of 2048 rows (0 to 2047, 2048 to 4095, ..., all dimensions but the last counted through in order) at most 384 rows name the same one
- block_counts: int32 [4, 8], P('col', 'tm'), may hold values from 1536 to 2048
- calibration: bfloat16 [16384, 4096], P('tm', 'col'), may hold values from -0.046875 to 0.046875
Outputs:
- calibrated: bfloat16 [4096, 4096], P('tm', 'col')
The draws below stay inside these ranges and needn't reach their ends.
Inputs may be any that keep to these rules, and one draw needn't show every extreme that they name: `block_owner`: among the 2048 block slots of one device, at most 384 name the same owner, a bound that some block reaches. The live blocks of device (tm t, col c) are its first block_counts[c, t] slots.
All inputs are finite; a program needn't handle non-finite values.
Results may differ from the reference program's by a relative error of at most 0.015.
Values may be sent and summed in bfloat16 or wider, within the bound.
A program may use at most 128 MiB of HBM per device.

```python
import math
import jax
import jax.numpy as jnp
import numpy as np
from jax import lax

SENSORS = 16384
OUTPUTS = 4096
BLOCK_LEN = 128
BLOCKS_DEV = 2048
WINDOWS = 4
CAPACITY = 384
GROUP_SENSORS = 4096
BLOCK_ROWS = 16384
GRID_ROWS = 4096
N_TM = 8
N_COL = 4


def plant(drawn, key, low, high):
    extent = drawn.shape
    index_at = [jax.random.randint(jax.random.fold_in(key, axis), (), 0, extent[axis]) for axis in range(len(extent))]
    drawn = drawn.at[tuple(index_at)].set(low)
    longest = extent.index(max(extent))
    index_at[longest] = (index_at[longest] + 1) % extent[longest]
    return drawn.at[tuple(index_at)].set(high)


def steps_of(key, dims, shards, low, top_value):
    level, own = 1.0, jax.random.fold_in(key, 6)
    for dim, blocks in shards:
        draws = jnp.exp(jax.random.uniform(jax.random.fold_in(own, dim), (blocks,), jnp.float32, low / len(shards), top_value / len(shards)))
        level = level * jnp.repeat(draws, dims[dim] // blocks).reshape([-1 if axis == dim else 1 for axis in range(len(dims))])
    return level


def deal_out(stream_key, own, number, rows, count, top, reach, slope):
    sequence = jax.random.permutation(stream_key, count)
    packed, usual = load_shares(count, rows * top, reach, slope, True), load_shares(count, rows * top, reach, slope, False)
    places = jnp.arange(count)

    def named(lengths, offset_by):
        used = int((lengths > 0).sum())
        fixed = max(1, used // 4)
        shifted = fixed + (places - fixed + offset_by * (used - fixed)) % max(1, count - fixed)
        return jnp.zeros((count,), jnp.int32).at[sequence[jnp.where(places < fixed, places, shifted)]].set(jnp.asarray(lengths, jnp.int32))

    lengths = jnp.where(number % 4 == 0, named(packed, number // 4), named(usual, number - number // 4 - 1))
    mixed = jax.random.permutation(jax.random.fold_in(own, 3), count)
    donor, sink = mixed[0:count // 2 * 2:2], mixed[1:count // 2 * 2:2]
    margin = jnp.minimum(lengths[donor] - 1, reach - lengths[sink]) // 2
    margin = jnp.where((donor == sequence[0]) | (sink == sequence[0]) | (lengths[sink] == 0), 0, jnp.maximum(margin, 0))
    shifted = jax.random.randint(jax.random.fold_in(own, 4), (count // 2,), 0, 1 << 20) % (margin + 1)
    lengths = lengths.at[donor].add(-shifted).at[sink].add(shifted)
    members = jnp.searchsorted(jnp.cumsum(lengths), jnp.arange(rows * top), side="right").astype(jnp.int32)
    grid = members.reshape(top, rows).T
    grid = grid[jax.random.permutation(jax.random.fold_in(own, 1), rows)]
    offset_by = jax.random.randint(jax.random.fold_in(own, 2), (rows, 1), 0, top)
    return jnp.take_along_axis(grid, (jnp.arange(top)[None, :] + offset_by) % top, axis=1)


def load_shares(count, total, bound, skew, full):
    portions = [(1 << 20) // math.isqrt(grade ** skew) + 1 for grade in range(1, count + 1)]
    largest = bound if full else min(bound, max(-(-total // count), total * portions[0] // sum(portions)))
    least = 1 if total - largest >= count - 1 else 0
    holding, spare = [largest] + [least] * (count - 1), total - largest - least * (count - 1)
    while spare > 0:
        free = [i for i in range(1, count) if holding[i] < largest] or [i for i in range(1, count) if holding[i] < bound]
        mass, remaining = sum([portions[i] for i in free]), spare
        for i in free:
            addition = min(bound - holding[i], max(1, remaining * portions[i] // mass), spare)
            holding[i] = holding[i] + addition
            spare = spare - addition
    return np.array(holding)


def gaussian(stream_key, extent, scale, bound, split=(), dtype=jnp.bfloat16):
    level = steps_of(stream_key, extent, split, -0.22, 0.18) if split else 1.0
    values = jax.random.normal(stream_key, extent, jnp.float32) * scale * level
    return jnp.minimum(jnp.maximum(values, -bound), bound).astype(dtype)


def setup_inputs(seed: int = 0) -> dict:
    key_of = jax.random.split(jax.random.key(seed), 8)
    block_values = gaussian(key_of[0], (N_COL, BLOCK_ROWS, BLOCK_LEN), 1.0, 6.0, ((0, 4), (1, 8)))
    block_shifts = jnp.clip(jax.random.uniform(key_of[1], (N_COL, BLOCK_ROWS, BLOCK_LEN), jnp.float32, -1.0, 1.0) * steps_of(key_of[1], (N_COL, BLOCK_ROWS, BLOCK_LEN), ((0, 4), (1, 8)), -0.4, 0.0), -1.0, 1.0).astype(jnp.bfloat16)
    block_sensor = plant(jax.random.randint(key_of[2], (N_COL, BLOCK_ROWS), 0, GROUP_SENSORS), jax.random.fold_in(key_of[2], 1), 0, GROUP_SENSORS - 1).astype(jnp.int32)
    block_window = plant(jax.random.randint(key_of[3], (N_COL, BLOCK_ROWS), 0, WINDOWS), jax.random.fold_in(key_of[3], 1), 0, WINDOWS - 1).astype(jnp.int32)
    block_owner_keys = jax.random.split(jax.random.fold_in(key_of[4], 1), N_COL * BLOCK_ROWS // BLOCKS_DEV)
    block_owner_turns = jax.random.permutation(jax.random.fold_in(key_of[4], 3), N_COL * BLOCK_ROWS // BLOCKS_DEV)
    block_owner = jax.vmap(lambda own, number: deal_out(jax.random.fold_in(key_of[4], 2), own, number, BLOCKS_DEV, N_TM, 1, CAPACITY, 2))(block_owner_keys, block_owner_turns).reshape((N_COL, BLOCK_ROWS, 1))
    block_counts = plant(jax.random.randint(key_of[5], (N_COL, N_TM), 3 * BLOCKS_DEV // 4, BLOCKS_DEV + 1), jax.random.fold_in(key_of[5], 1), 3 * BLOCKS_DEV // 4, BLOCKS_DEV).astype(jnp.int32)
    calibration = gaussian(key_of[6], (SENSORS, OUTPUTS), SENSORS ** -0.5, 0.046875, ((0, 8), (1, 4)))
    return dict(block_values=block_values, block_shifts=block_shifts, block_sensor=block_sensor, block_window=block_window, block_owner=block_owner, block_counts=block_counts, calibration=calibration)


def spread_samples(values, shifts):
    samples = values.astype(jnp.float32)
    offsets = shifts.astype(jnp.float32)
    result = jnp.zeros(samples.shape, jnp.float32)
    lead = [(0, 0)] * (samples.ndim - 1)
    for displace in (-1, 0, 1):
        weight = jnp.maximum(0.0, 1.0 - jnp.abs(offsets - displace)).astype(jnp.bfloat16)
        weight = lax.optimization_barrier(weight).astype(jnp.float32)
        product = weight * samples
        if displace == 1:
            result = result + jnp.pad(product[..., :-1], lead + [(1, 0)])
        elif displace == -1:
            result = result + jnp.pad(product[..., 1:], lead + [(0, 1)])
        else:
            result = result + product
    return result


def reference(block_values, block_shifts, block_sensor, block_window, block_owner, block_counts, calibration):
    length = block_values.shape[2]
    local_index = lax.broadcasted_iota(jnp.int32, (N_COL, BLOCK_ROWS), 1) % BLOCKS_DEV
    counts_rep = jnp.repeat(block_counts, BLOCKS_DEV, axis=1)
    is_live = (local_index < counts_rep).astype(jnp.float32)
    contribution = spread_samples(block_values, block_shifts) * is_live[:, :, None]
    col_base = lax.broadcasted_iota(jnp.int32, (N_COL, BLOCK_ROWS), 0) * GROUP_SENSORS
    row_keys = (block_owner[:, :, 0] * WINDOWS + block_window) * SENSORS + col_base + block_sensor
    summed = jnp.zeros((N_TM * WINDOWS * SENSORS, length), jnp.float32)
    summed = summed.at[row_keys.reshape(-1)].add(contribution.reshape(-1, length))
    aligned = summed.reshape(N_TM * WINDOWS, SENSORS, length).transpose(0, 2, 1)
    aligned = aligned.reshape(GRID_ROWS, SENSORS).astype(jnp.bfloat16)
    return jnp.dot(aligned, calibration, preferred_element_type=jnp.float32).astype(jnp.bfloat16)
```

```python
import functools

import jax
import jax.numpy as jnp
from jax import lax
from jax.experimental import pallas as pl
from jax.experimental.pallas import tpu as pltpu
from jax.sharding import PartitionSpec as P

ROWS_DEV = 512
CHUNK = 256
UNROLL = 8


def spread_samples(values, shifts):
    samples = values.astype(jnp.float32)
    offsets = shifts.astype(jnp.float32)
    result = jnp.zeros(samples.shape, jnp.float32)
    lead = [(0, 0)] * (samples.ndim - 1)
    for displace in (-1, 0, 1):
        weight = jnp.maximum(0.0, 1.0 - jnp.abs(offsets - displace)).astype(jnp.bfloat16)
        weight = lax.optimization_barrier(weight).astype(jnp.float32)
        product = weight * samples
        if displace == 1:
            result = result + jnp.pad(product[..., :-1], lead + [(1, 0)])
        elif displace == -1:
            result = jnp.pad(product[..., 1:], lead + [(0, 1)])
        else:
            result = result + product
    return result


def project_kernel(
    cfg, sens_ref, off_ref, contrib_hbm, *rest
):
    parts, sources, stride, rows, bins, capacity = cfg
    calib_hbm = rest[:parts]
    out_ref = rest[parts]
    contrib_bf, contrib, calib, gathered, picked, total, sems = rest[parts + 1:]
    copies = [pltpu.make_async_copy(contrib_hbm, contrib_bf, sems.at[parts])]
    for part in range(parts):
        copies.append(
            pltpu.make_async_copy(
                calib_hbm[part], calib.at[pl.ds(part * rows, rows)], sems.at[part]
            )
        )
    for copy in copies:
        copy.start()
    width = calib.shape[1]
    room = gathered.shape[0]
    gathered[...] = jnp.zeros_like(gathered)
    picked[...] = jnp.zeros_like(picked)
    copies[0].wait()
    piece = 256
    whole = sources * stride // piece

    def widen(step, carry):
        at = pl.ds(pl.multiple_of(step * piece, piece), piece)
        contrib[at, :] = contrib_bf[at, :].astype(jnp.float32)
        return carry

    lax.fori_loop(0, whole, widen, 0)
    if whole * piece < sources * stride:
        tail = pl.ds(whole * piece, sources * stride - whole * piece)
        contrib[tail, :] = contrib_bf[tail, :].astype(jnp.float32)
    for copy in copies[1:]:
        copy.wait()

    def flush(count):
        def chunk(step, carry):
            start = pl.multiple_of(step * CHUNK, CHUNK)
            row = lax.broadcasted_iota(jnp.int32, (CHUNK, picked.shape[1]), 0) + start
            left = jnp.where(row < count, picked[pl.ds(start, CHUNK), :], 0.0).astype(jnp.bfloat16)
            right = jnp.concatenate(
                [gathered[pl.ds(start, CHUNK), lane, :].astype(jnp.bfloat16) for lane in range(width)],
                axis=1,
            )
            total[...] += lax.dot_general(
                left, right, (((0,), (0,)), ((), ())), preferred_element_type=jnp.float32
            )
            return carry

        lax.fori_loop(0, (count + CHUNK - 1) // CHUNK, chunk, 0)

    def window(w, carry):
        total[...] = jnp.zeros_like(total)

        def source(src, count):
            begin = off_ref[src * (bins + 1) + w]
            end = off_ref[src * (bins + 1) + w + 1]
            base = src * stride + begin

            def copy_rows(step, inner):
                for lane in range(UNROLL):
                    at = step * UNROLL + lane
                    sensor = sens_ref[base + at]
                    gathered[count + at] = calib[sensor].astype(jnp.float32)
                    picked[pl.ds(count + at, 1), :] = contrib[pl.ds(base + at, 1), :]
                return inner

            lax.fori_loop(0, (end - begin + UNROLL - 1) // UNROLL, copy_rows, 0)
            count = count + end - begin
            full = count + capacity + UNROLL > room

            @pl.when(full)
            def _():
                flush(count)

            return jnp.where(full, 0, count)

        count = lax.fori_loop(0, sources, source, 0)
        flush(count)
        out_ref[pl.ds(pl.multiple_of(w * 128, 128), 128), :] = total[...].astype(out_ref.dtype)
        return carry

    lax.fori_loop(0, bins, window, 0)


def per_device(
    block_values, block_shifts, block_sensor, block_window, block_owner, block_counts, calibration
):
    values = block_values[0]
    blocks, length = values.shape
    owners = lax.axis_size("tm")
    cols = lax.axis_size("col")
    ratio = owners // cols
    windows = ROWS_DEV // length
    rows, outputs = calibration.shape
    lanes = outputs // 128
    capacity = min(blocks, blocks * 3 // (2 * owners))
    me = lax.axis_index("tm")
    lot = me % ratio

    calib = lax.optimization_barrier(calibration.reshape(rows, lanes, 128))
    calib_parts = [calib]
    for step in range(1, ratio):
        pairs = [
            ((t // ratio) * ratio + (t + step) % ratio, t) for t in range(owners)
        ]
        calib_parts.append(lax.ppermute(calib, "tm", pairs))

    contribution = spread_samples(values, block_shifts[0]).astype(jnp.bfloat16)
    block_index = lax.iota(jnp.int32, blocks)
    is_live = block_index < block_counts[0, 0]
    owner = block_owner[0, :, 0]
    per_lot = owners // ratio * windows
    bin_of = (owner % ratio) * per_lot + (owner // ratio) * windows + block_window[0]
    bin_of = jnp.where(is_live, bin_of, owners * windows)
    order = bin_of * blocks + block_index
    rank = jnp.sum((order[None, :] < order[:, None]).astype(jnp.int32), axis=1)
    place = (rank[None, :] == block_index[:, None]).astype(jnp.bfloat16)
    sensor = block_sensor[0]
    payload = jnp.concatenate(
        (
            contribution,
            (sensor // 128).astype(jnp.bfloat16)[:, None],
            (sensor % 128).astype(jnp.bfloat16)[:, None],
            jnp.zeros((blocks, length - 2), jnp.bfloat16),
        ),
        axis=1,
    )
    placed = jnp.dot(place, payload, preferred_element_type=jnp.float32)
    bounds = jnp.sum(
        (bin_of[None, :] < lax.iota(jnp.int32, owners * windows + 1)[:, None]).astype(jnp.int32), axis=1
    )
    bound_rows = -(-(owners * windows + 1) // length)
    bounds = jnp.pad(bounds, (0, bound_rows * length - bounds.shape[0]))
    extra = jnp.concatenate(
        (
            placed[:, length].reshape(-1, length),
            placed[:, length + 1].reshape(-1, length),
            (bounds // 128).astype(jnp.float32).reshape(-1, length),
            (bounds % 128).astype(jnp.float32).reshape(-1, length),
        ),
        axis=0,
    )
    extra_rows = -(-extra.shape[0] // 16) * 16
    extra = jnp.pad(extra, ((0, extra_rows - extra.shape[0]), (0, 0)))
    parcel = jnp.concatenate((placed[:, :length], extra), axis=0).astype(jnp.bfloat16)
    stride = blocks + extra_rows
    swap = [
        (t * cols + c, (c * ratio + t % ratio) * cols + t // ratio)
        for t in range(owners)
        for c in range(cols)
    ]
    parcel = lax.ppermute(parcel, ("tm", "col"), swap)
    steps = [parcel]
    for step in range(1, ratio):
        pairs = [
            ((t // ratio) * ratio + (t + step) % ratio, t) for t in range(owners)
        ]
        steps.append(lax.ppermute(parcel, "tm", pairs))
    bundle = jnp.concatenate(steps, axis=0)
    bundle = lax.all_gather(bundle, "col", axis=0, tiled=True)
    sources = owners

    meta = bundle.reshape(sources, stride, length)[:, blocks:].astype(jnp.int32)
    third = blocks // length
    sensors = (meta[:, :third] * 128 + meta[:, third:2 * third]).reshape(sources, blocks)
    sensors = ((sensors // rows - lot) % ratio) * rows + sensors % rows
    sensors = jnp.pad(sensors, ((0, 0), (0, extra_rows))).reshape(-1)
    limit = (
        meta[:, 2 * third:2 * third + bound_rows] * 128
        + meta[:, 2 * third + bound_rows:2 * third + 2 * bound_rows]
    ).reshape(sources, bound_rows * length)
    limit = lax.dynamic_slice_in_dim(limit, lot * per_lot, per_lot + 1, axis=1).reshape(-1)

    room = -(-(CHUNK * 4 + capacity + 2 * UNROLL) // CHUNK) * CHUNK
    total_rows = sources * stride
    any_space = pl.BlockSpec(memory_space=pl.ANY)
    smem = pl.BlockSpec(memory_space=pltpu.SMEM)
    cfg = (ratio, sources, stride, rows, per_lot, capacity)
    partial = pl.pallas_call(
        functools.partial(project_kernel, cfg),
        out_shape=jax.ShapeDtypeStruct((per_lot * length, outputs), jnp.bfloat16),
        in_specs=[smem, smem, any_space] + [any_space] * ratio,
        out_specs=pl.BlockSpec(memory_space=pltpu.VMEM),
        scratch_shapes=[
            pltpu.VMEM((total_rows, length), jnp.bfloat16),
            pltpu.VMEM((total_rows, length), jnp.float32),
            pltpu.VMEM((ratio * rows, lanes, 128), jnp.bfloat16),
            pltpu.VMEM((room, lanes, 128), jnp.float32),
            pltpu.VMEM((room, length), jnp.float32),
            pltpu.VMEM((length, outputs), jnp.float32),
            pltpu.SemaphoreType.DMA((ratio + 1,)),
        ],
        compiler_params=pltpu.CompilerParams(vmem_limit_bytes=60 * 1024 * 1024),
        cost_estimate=pl.CostEstimate(flops=6 * 10**9, bytes_accessed=40 * 10**6, transcendentals=0),
    )(sensors, limit, bundle, *calib_parts)
    groups = [[t for t in range(owners) if t % ratio == p] for p in range(ratio)]
    return lax.psum_scatter(
        partial, "tm", scatter_dimension=0, axis_index_groups=groups, tiled=True
    )


def solution(mesh):
    placed = (
        P("col", "tm", None),
        P("col", "tm", None),
        P("col", "tm"),
        P("col", "tm"),
        P("col", "tm", None),
        P("col", "tm"),
        P("tm", "col"),
    )
    return jax.shard_map(
        per_device, mesh=mesh, in_specs=placed, out_specs=P("tm", "col"), check_vma=False
    )
```

```python
import functools

import jax
import jax.numpy as jnp
from jax import lax
from jax.experimental import pallas as pl
from jax.experimental.pallas import tpu as pltpu
from jax.sharding import PartitionSpec as P


ROWS_DEV = 512
CHUNK = 256
UNROLL = 8
PIECES = 2


def spread_samples(values, shifts):
    samples = values.astype(jnp.float32)
    offsets = shifts.astype(jnp.float32)
    result = jnp.zeros(samples.shape, jnp.float32)
    lead = [(0, 0)] * (samples.ndim - 1)
    for displace in (-1, 0, 1):
        weight = jnp.maximum(0.0, 1.0 - jnp.abs(offsets - displace)).astype(jnp.bfloat16)
        weight = lax.optimization_barrier(weight).astype(jnp.float32)
        product = weight * samples
        if displace == 1:
            result = result + jnp.pad(product[..., :-1], lead + [(1, 0)])
        elif displace == -1:
            result = jnp.pad(product[..., 1:], lead + [(0, 1)])
        else:
            result = result + product
    return result


def project_kernel(cfg, sens_ref, off_ref, *rest):
    sources, stride, heights, windows, owners, pieces, seeded, capacity = cfg
    bins = windows * owners
    share = windows // PIECES
    contrib_hbm, rest = rest[:sources], rest[sources:]
    calib_hbm, rest = rest[:len(heights)], rest[len(heights):]
    seed_refs, rest = (rest[:len(pieces)], rest[len(pieces):]) if seeded else ((), rest)
    out_refs, rest = rest[:len(pieces)], rest[len(pieces):]
    contrib_bf, contrib, calib, gathered, picked, total, sems = rest
    copies = []
    for src in range(sources):
        copies.append(
            pltpu.make_async_copy(
                contrib_hbm[src], contrib_bf.at[pl.ds(src * stride, stride)], sems.at[src]
            )
        )
    at = 0
    for part, height in enumerate(heights):
        copies.append(
            pltpu.make_async_copy(
                calib_hbm[part], calib.at[pl.ds(at, height)], sems.at[sources + part]
            )
        )
        at += height
    for copy in copies:
        copy.start()
    width = calib.shape[1]
    room = gathered.shape[0]
    gathered[...] = jnp.zeros_like(gathered)
    picked[...] = jnp.zeros_like(picked)
    for copy in copies[:sources]:
        copy.wait()

    def widen(step, carry):
        at = pl.ds(pl.multiple_of(step * stride, 16), stride)
        contrib[at, :] = contrib_bf[at, :].astype(jnp.float32)
        return carry

    lax.fori_loop(0, sources, widen, 0)
    for copy in copies[sources:]:
        copy.wait()

    def flush(count):
        def chunk(step, carry):
            start = pl.multiple_of(step * CHUNK, CHUNK)
            row = lax.broadcasted_iota(jnp.int32, (CHUNK, picked.shape[1]), 0) + start
            left = jnp.where(row < count, picked[pl.ds(start, CHUNK), :], 0.0).astype(jnp.bfloat16)
            right = jnp.concatenate(
                [gathered[pl.ds(start, CHUNK), lane, :].astype(jnp.bfloat16) for lane in range(width)],
                axis=1,
            )
            total[...] += lax.dot_general(
                left, right, (((0,), (0,)), ((), ())), preferred_element_type=jnp.float32
            )
            return carry

        lax.fori_loop(0, (count + CHUNK - 1) // CHUNK, chunk, 0)

    for number, index in enumerate(pieces):

        def window(slot, carry, number=number, index=index):
            w = (slot // share) * windows + index * share + slot % share
            rows_at = pl.ds(pl.multiple_of(slot * 128, 128), 128)
            if seeded:
                total[...] = seed_refs[number][rows_at, :]
            else:
                total[...] = jnp.zeros_like(total)

            def source(src, count):
                begin = off_ref[src * (bins + 1) + w]
                end = off_ref[src * (bins + 1) + w + 1]
                base = src * stride + begin

                def copy_rows(step, inner):
                    for lane in range(UNROLL):
                        at = step * UNROLL + lane
                        sensor = sens_ref[base + at]
                        gathered[count + at] = calib[sensor].astype(jnp.float32)
                        picked[pl.ds(count + at, 1), :] = contrib[pl.ds(base + at, 1), :]
                    return inner

                lax.fori_loop(0, (end - begin + UNROLL - 1) // UNROLL, copy_rows, 0)
                count = count + end - begin
                full = count + capacity + UNROLL > room

                @pl.when(full)
                def _():
                    flush(count)

                return jnp.where(full, 0, count)

            flush(lax.fori_loop(0, sources, source, 0))
            out_refs[number][rows_at, :] = total[...].astype(out_refs[number].dtype)
            return carry

        lax.fori_loop(0, owners * share, window, 0)


def project(sensors, limit, parcels, calibs, seeds, pieces, windows, owners, capacity, dtype):
    stride, length = parcels[0].shape
    sources = len(parcels)
    lanes = calibs[0].shape[1]
    outputs = lanes * 128
    heights = tuple(c.shape[0] for c in calibs)
    room = -(-(CHUNK * 4 + capacity + 2 * UNROLL) // CHUNK) * CHUNK
    height = windows // PIECES * owners * length
    any_space = pl.BlockSpec(memory_space=pl.ANY)
    smem = pl.BlockSpec(memory_space=pltpu.SMEM)
    vmem = pl.BlockSpec(memory_space=pltpu.VMEM)
    cfg = (sources, stride, heights, windows, owners, pieces, bool(seeds), capacity)
    return pl.pallas_call(
        functools.partial(project_kernel, cfg),
        out_shape=[jax.ShapeDtypeStruct((height, outputs), dtype)] * len(pieces),
        in_specs=[smem, smem] + [any_space] * (sources + len(calibs)) + [vmem] * len(seeds),
        out_specs=[vmem] * len(pieces),
        scratch_shapes=[
            pltpu.VMEM((sources * stride, length), jnp.bfloat16),
            pltpu.VMEM((sources * stride, length), jnp.float32),
            pltpu.VMEM((sum(heights), lanes, 128), jnp.bfloat16),
            pltpu.VMEM((room, lanes, 128), jnp.float32),
            pltpu.VMEM((room, length), jnp.float32),
            pltpu.VMEM((length, outputs), jnp.float32),
            pltpu.SemaphoreType.DMA((sources + len(calibs),)),
        ],
        compiler_params=pltpu.CompilerParams(vmem_limit_bytes=58 * 1024 * 1024),
        cost_estimate=pl.CostEstimate(
            flops=15 * 10**9 * len(pieces), bytes_accessed=20 * 10**6, transcendentals=0
        ),
    )(sensors, limit, *parcels, *calibs, *seeds)


def resample(
    block_values, block_shifts, block_sensor, block_window, block_owner, block_counts, calibration
):
    values = block_values[0]
    blocks, length = values.shape
    owners = lax.axis_size("tm")
    cols = lax.axis_size("col")
    ratio = owners // cols
    windows = ROWS_DEV // length
    rows, outputs = calibration.shape
    lanes = outputs // 128
    capacity = min(blocks, blocks * 3 // (2 * owners))
    lot = lax.axis_index("tm") % ratio

    def shifted(step):
        return [((t // ratio) * ratio + (t + step) % ratio, t) for t in range(owners)]

    calib = lax.optimization_barrier(calibration.reshape(rows, lanes, 128))
    early = rows // 4
    calib_early = []
    for step in range(1, ratio):
        calib_early.append(lax.ppermute(calib[:early], "tm", shifted(step)))

    contribution = spread_samples(values, block_shifts[0]).astype(jnp.bfloat16)
    block_index = lax.iota(jnp.int32, blocks)
    is_live = block_index < block_counts[0, 0]
    owner = block_owner[0, :, 0]
    sensor = block_sensor[0]
    held = owners // ratio
    per_lot = held * windows
    bins = ratio * ratio * per_lot
    bin_of = ((owner % ratio) * ratio + sensor // rows) * per_lot
    bin_of = bin_of + (owner // ratio) * windows + block_window[0]
    bin_of = jnp.where(is_live, bin_of, bins)
    order = bin_of * blocks + block_index
    rank = jnp.sum((order[None, :] < order[:, None]).astype(jnp.int32), axis=1)
    place = (rank[None, :] == block_index[:, None]).astype(jnp.bfloat16)
    payload = jnp.concatenate(
        (
            contribution,
            (sensor // 128).astype(jnp.bfloat16)[:, None],
            (sensor % 128).astype(jnp.bfloat16)[:, None],
            jnp.zeros((blocks, length - 2), jnp.bfloat16),
        ),
        axis=1,
    )
    placed = jnp.dot(place, payload, preferred_element_type=jnp.float32)
    bounds = jnp.sum(
        (bin_of[None, :] < lax.iota(jnp.int32, bins + 1)[:, None]).astype(jnp.int32), axis=1
    )
    bound_rows = -(-(bins + 1) // length)
    bounds = jnp.pad(bounds, (0, bound_rows * length - bounds.shape[0]))
    extra = jnp.concatenate(
        (
            placed[:, length].reshape(-1, length),
            placed[:, length + 1].reshape(-1, length),
            (bounds // 128).astype(jnp.float32).reshape(-1, length),
            (bounds % 128).astype(jnp.float32).reshape(-1, length),
        ),
        axis=0,
    )
    extra_rows = -(-extra.shape[0] // 16) * 16
    extra = jnp.pad(extra, ((0, extra_rows - extra.shape[0]), (0, 0)))
    parcel = jnp.concatenate((placed[:, :length], extra), axis=0).astype(jnp.bfloat16)
    swap = [
        (t * cols + c, (c * ratio + t % ratio) * cols + t // ratio)
        for t in range(owners)
        for c in range(cols)
    ]
    parcel = lax.ppermute(parcel, ("tm", "col"), swap)
    parcels = [parcel]
    for step in range(1, ratio):
        parcels.append(lax.ppermute(parcel, "tm", shifted(step)))
    calib_late, last = lax.optimization_barrier((calib[early:], parcels[-1]))
    parcels[-1] = last
    calib_rest = []
    for step in range(1, ratio):
        calib_rest.append(lax.ppermute(calib_late, "tm", shifted(step)))
    bit = 2
    while bit < cols:
        pairs = [(c, c ^ bit) for c in range(cols)]
        parcels += [lax.ppermute(p, "col", pairs) for p in parcels]
        bit *= 2
    pairs = [(c, c ^ 1) for c in range(cols)]
    parcels += [lax.ppermute(p, "col", pairs) for p in parcels]
    sources = len(parcels)

    meta = jnp.stack([p[blocks:] for p in parcels]).astype(jnp.int32)
    third = blocks // length
    sensors = (meta[:, :third] * 128 + meta[:, third:2 * third]).reshape(sources, blocks) % rows
    sensors = jnp.pad(sensors, ((0, 0), (0, extra_rows))).reshape(-1)
    limit = (
        meta[:, 2 * third:2 * third + bound_rows] * 128
        + meta[:, 2 * third + bound_rows:2 * third + 2 * bound_rows]
    ).reshape(sources, bound_rows * length)

    def limit_of(step):
        first = (lot * ratio + (lot + step) % ratio) * per_lot
        return lax.dynamic_slice_in_dim(limit, first, per_lot + 1, axis=1).reshape(-1)

    every = tuple(range(PIECES))
    partial = project(
        sensors, limit_of(0), parcels, [calib], [], every, windows, held, capacity, jnp.float32
    )
    groups = [[t for t in range(owners) if t % ratio == p] for p in range(ratio)]
    results = []
    for piece in every:
        held_sum = partial[piece]
        for step in range(1, ratio):
            kind = jnp.bfloat16 if step == ratio - 1 else jnp.float32
            held_sum = project(
                sensors, limit_of(step), parcels, [calib_early[step - 1], calib_rest[step - 1]],
                [held_sum], (piece,), windows, held, capacity, kind
            )[0]
        results.append(
            lax.psum_scatter(
                held_sum, "tm", scatter_dimension=0, axis_index_groups=groups, tiled=True
            )
        )
    return jnp.concatenate(results, axis=0)


def solution(mesh):
    placed = (
        P("col", "tm", None),
        P("col", "tm", None),
        P("col", "tm"),
        P("col", "tm"),
        P("col", "tm", None),
        P("col", "tm"),
        P("tm", "col"),
    )
    return jax.shard_map(
        resample, mesh=mesh, in_specs=placed, out_specs=P("tm", "col"), check_vma=False
    )
```

```python
import functools

import jax
import jax.numpy as jnp
from jax import lax
from jax.experimental import pallas as pl
from jax.experimental.pallas import tpu as pltpu
from jax.sharding import PartitionSpec as P


ROWS_DEV = 512
CHUNK = 256
UNROLL = 8
PITCH = 8
PIECES = 2


def spread_samples(values, shifts):
    samples = values.astype(jnp.float32)
    offsets = shifts.astype(jnp.float32)
    result = jnp.zeros(samples.shape, jnp.float32)
    lead = [(0, 0)] * (samples.ndim - 1)
    for displace in (-1, 0, 1):
        weight = jnp.maximum(0.0, 1.0 - jnp.abs(offsets - displace)).astype(jnp.bfloat16)
        weight = lax.optimization_barrier(weight).astype(jnp.float32)
        product = weight * samples
        if displace == 1:
            result = result + jnp.pad(product[..., :-1], lead + [(1, 0)])
        elif displace == -1:
            result = jnp.pad(product[..., 1:], lead + [(0, 1)])
        else:
            result = result + product
    return result


def project_kernel(cfg, sens_ref, off_ref, *rest):
    sources, stride, heights, windows, owners, pieces, seeded, capacity = cfg
    bins = windows * owners
    share = windows // PIECES
    contrib_hbm, rest = rest[:sources], rest[sources:]
    calib_hbm, rest = rest[:len(heights)], rest[len(heights):]
    seed_refs, rest = (rest[:len(pieces)], rest[len(pieces):]) if seeded else ((), rest)
    out_refs, rest = rest[:len(pieces)], rest[len(pieces):]
    contrib_bf, contrib, calib, gathered, picked, total, sems = rest
    copies = []
    for src in range(sources):
        copies.append(
            pltpu.make_async_copy(
                contrib_hbm[src], contrib_bf.at[pl.ds(src * stride, stride)], sems.at[src]
            )
        )
    at = 0
    for part, height in enumerate(heights):
        copies.append(
            pltpu.make_async_copy(
                calib_hbm[part], calib.at[pl.ds(at, height)], sems.at[sources + part]
            )
        )
        at += height
    for copy in copies:
        copy.start()
    width = calib.shape[1]
    room = picked.shape[0]
    gathered[...] = jnp.zeros_like(gathered)
    picked[...] = jnp.zeros_like(picked)
    for copy in copies[:sources]:
        copy.wait()

    def widen(step, carry):
        at = pl.ds(pl.multiple_of(step * stride, 16), stride)
        contrib[at, :] = contrib_bf[at, :].astype(jnp.float32)
        return carry

    lax.fori_loop(0, sources, widen, 0)
    for copy in copies[sources:]:
        copy.wait()

    def flush(count):
        def chunk(step, carry):
            start = pl.multiple_of(step * CHUNK, CHUNK)
            row = lax.broadcasted_iota(jnp.int32, (CHUNK, picked.shape[1]), 0) + start
            left = jnp.where(row < count, picked[pl.ds(start, CHUNK), :], 0.0).astype(jnp.bfloat16)
            right = jnp.concatenate(
                [
                    gathered[pl.ds(start * PITCH + lane, CHUNK, stride=PITCH), :].astype(jnp.bfloat16)
                    for lane in range(width)
                ],
                axis=1,
            )
            total[...] += lax.dot_general(
                left, right, (((0,), (0,)), ((), ())), preferred_element_type=jnp.float32
            )
            return carry

        lax.fori_loop(0, (count + CHUNK - 1) // CHUNK, chunk, 0)

    for number, index in enumerate(pieces):

        def window(slot, carry, number=number, index=index):
            w = (slot // share) * windows + index * share + slot % share
            rows_at = pl.ds(pl.multiple_of(slot * 128, 128), 128)
            if seeded:
                total[...] = seed_refs[number][rows_at, :]
            else:
                total[...] = jnp.zeros_like(total)

            def source(src, count):
                begin = off_ref[src * (bins + 1) + w]
                end = off_ref[src * (bins + 1) + w + 1]
                base = src * stride + begin

                def copy_rows(step, inner):
                    for lane in range(UNROLL):
                        at = step * UNROLL + lane
                        sensor = sens_ref[base + at]
                        spot = pl.multiple_of((count + at) * PITCH, PITCH)
                        gathered[pl.ds(spot, width), :] = calib[sensor].astype(jnp.float32)
                        picked[pl.ds(count + at, 1), :] = contrib[pl.ds(base + at, 1), :]
                    return inner

                lax.fori_loop(0, (end - begin + UNROLL - 1) // UNROLL, copy_rows, 0)
                count = count + end - begin
                full = count + capacity + UNROLL > room

                @pl.when(full)
                def _():
                    flush(count)

                return jnp.where(full, 0, count)

            flush(lax.fori_loop(0, sources, source, 0))
            out_refs[number][rows_at, :] = total[...].astype(out_refs[number].dtype)
            return carry

        lax.fori_loop(0, owners * share, window, 0)


def project(sensors, limit, parcels, calibs, seeds, pieces, windows, owners, capacity, dtype):
    stride, length = parcels[0].shape
    sources = len(parcels)
    lanes = calibs[0].shape[1]
    outputs = lanes * 128
    heights = tuple(c.shape[0] for c in calibs)
    room = -(-(CHUNK * 4 + capacity + 2 * UNROLL) // CHUNK) * CHUNK
    height = windows // PIECES * owners * length
    any_space = pl.BlockSpec(memory_space=pl.ANY)
    smem = pl.BlockSpec(memory_space=pltpu.SMEM)
    vmem = pl.BlockSpec(memory_space=pltpu.VMEM)
    cfg = (sources, stride, heights, windows, owners, pieces, bool(seeds), capacity)
    return pl.pallas_call(
        functools.partial(project_kernel, cfg),
        out_shape=[jax.ShapeDtypeStruct((height, outputs), dtype)] * len(pieces),
        in_specs=[smem, smem] + [any_space] * (sources + len(calibs)) + [vmem] * len(seeds),
        out_specs=[vmem] * len(pieces),
        scratch_shapes=[
            pltpu.VMEM((sources * stride, length), jnp.bfloat16),
            pltpu.VMEM((sources * stride, length), jnp.float32),
            pltpu.VMEM((sum(heights), lanes, 128), jnp.bfloat16),
            pltpu.VMEM((room * PITCH, 128), jnp.float32),
            pltpu.VMEM((room, length), jnp.float32),
            pltpu.VMEM((length, outputs), jnp.float32),
            pltpu.SemaphoreType.DMA((sources + len(calibs),)),
        ],
        compiler_params=pltpu.CompilerParams(vmem_limit_bytes=58 * 1024 * 1024),
        cost_estimate=pl.CostEstimate(
            flops=15 * 10**9 * len(pieces), bytes_accessed=20 * 10**6, transcendentals=0
        ),
    )(sensors, limit, *parcels, *calibs, *seeds)


def resample(
    block_values, block_shifts, block_sensor, block_window, block_owner, block_counts, calibration
):
    values = block_values[0]
    blocks, length = values.shape
    owners = lax.axis_size("tm")
    cols = lax.axis_size("col")
    ratio = owners // cols
    windows = ROWS_DEV // length
    rows, outputs = calibration.shape
    lanes = outputs // 128
    capacity = min(blocks, blocks * 3 // (2 * owners))
    lot = lax.axis_index("tm") % ratio

    def shifted(step):
        return [((t // ratio) * ratio + (t + step) % ratio, t) for t in range(owners)]

    calib = lax.optimization_barrier(calibration.reshape(rows, lanes, 128))
    early = rows // 4
    calib_early = []
    for step in range(1, ratio):
        calib_early.append(lax.ppermute(calib[:early], "tm", shifted(step)))

    contribution = spread_samples(values, block_shifts[0]).astype(jnp.bfloat16)
    block_index = lax.iota(jnp.int32, blocks)
    is_live = block_index < block_counts[0, 0]
    owner = block_owner[0, :, 0]
    sensor = block_sensor[0]
    held = owners // ratio
    per_lot = held * windows
    bins = ratio * ratio * per_lot
    bin_of = ((owner % ratio) * ratio + sensor // rows) * per_lot
    bin_of = bin_of + (owner // ratio) * windows + block_window[0]
    bin_of = jnp.where(is_live, bin_of, bins)
    order = bin_of * blocks + block_index
    rank = jnp.sum((order[None, :] < order[:, None]).astype(jnp.int32), axis=1)
    place = (rank[None, :] == block_index[:, None]).astype(jnp.bfloat16)
    payload = jnp.concatenate(
        (
            contribution,
            (sensor // 128).astype(jnp.bfloat16)[:, None],
            (sensor % 128).astype(jnp.bfloat16)[:, None],
            jnp.zeros((blocks, length - 2), jnp.bfloat16),
        ),
        axis=1,
    )
    placed = jnp.dot(place, payload, preferred_element_type=jnp.float32)
    bounds = jnp.sum(
        (bin_of[None, :] < lax.iota(jnp.int32, bins + 1)[:, None]).astype(jnp.int32), axis=1
    )
    bound_rows = -(-(bins + 1) // length)
    bounds = jnp.pad(bounds, (0, bound_rows * length - bounds.shape[0]))
    extra = jnp.concatenate(
        (
            placed[:, length].reshape(-1, length),
            placed[:, length + 1].reshape(-1, length),
            (bounds // 128).astype(jnp.float32).reshape(-1, length),
            (bounds % 128).astype(jnp.float32).reshape(-1, length),
        ),
        axis=0,
    )
    extra_rows = -(-extra.shape[0] // 16) * 16
    extra = jnp.pad(extra, ((0, extra_rows - extra.shape[0]), (0, 0)))
    parcel = jnp.concatenate((placed[:, :length], extra), axis=0).astype(jnp.bfloat16)
    swap = [
        (t * cols + c, (c * ratio + t % ratio) * cols + t // ratio)
        for t in range(owners)
        for c in range(cols)
    ]
    parcel = lax.ppermute(parcel, ("tm", "col"), swap)
    parcels = [parcel]
    for step in range(1, ratio):
        parcels.append(lax.ppermute(parcel, "tm", shifted(step)))
    calib_late, last = lax.optimization_barrier((calib[early:], parcels[-1]))
    parcels[-1] = last
    calib_rest = []
    for step in range(1, ratio):
        calib_rest.append(lax.ppermute(calib_late, "tm", shifted(step)))
    bit = 2
    while bit < cols:
        pairs = [(c, c ^ bit) for c in range(cols)]
        parcels += [lax.ppermute(p, "col", pairs) for p in parcels]
        bit *= 2
    pairs = [(c, c ^ 1) for c in range(cols)]
    parcels += [lax.ppermute(p, "col", pairs) for p in parcels]
    sources = len(parcels)

    meta = jnp.stack([p[blocks:] for p in parcels]).astype(jnp.int32)
    third = blocks // length
    sensors = (meta[:, :third] * 128 + meta[:, third:2 * third]).reshape(sources, blocks) % rows
    sensors = jnp.pad(sensors, ((0, 0), (0, extra_rows))).reshape(-1)
    limit = (
        meta[:, 2 * third:2 * third + bound_rows] * 128
        + meta[:, 2 * third + bound_rows:2 * third + 2 * bound_rows]
    ).reshape(sources, bound_rows * length)

    def limit_of(step):
        first = (lot * ratio + (lot + step) % ratio) * per_lot
        return lax.dynamic_slice_in_dim(limit, first, per_lot + 1, axis=1).reshape(-1)

    every = tuple(range(PIECES))
    partial = project(
        sensors, limit_of(0), parcels, [calib], [], every, windows, held, capacity, jnp.float32
    )
    groups = [[t for t in range(owners) if t % ratio == p] for p in range(ratio)]
    results = []
    for piece in every:
        held_sum = partial[piece]
        for step in range(1, ratio):
            kind = jnp.bfloat16 if step == ratio - 1 else jnp.float32
            held_sum = project(
                sensors, limit_of(step), parcels, [calib_early[step - 1], calib_rest[step - 1]],
                [held_sum], (piece,), windows, held, capacity, kind
            )[0]
        results.append(
            lax.psum_scatter(
                held_sum, "tm", scatter_dimension=0, axis_index_groups=groups, tiled=True
            )
        )
    return jnp.concatenate(results, axis=0)


def solution(mesh):
    placed = (
        P("col", "tm", None),
        P("col", "tm", None),
        P("col", "tm"),
        P("col", "tm"),
        P("col", "tm", None),
        P("col", "tm"),
        P("tm", "col"),
    )
    return jax.shard_map(
        resample, mesh=mesh, in_specs=placed, out_specs=P("tm", "col"), check_vma=False
    )
```
